32 devices in a mesh: slab: 8 (over z, y), energy: 4 (over x, core).
Axes of the slice: x: 2, y: 2, z: 4, core: 2. Of those that a mesh axis runs over, the one named last changes fastest.
Arguments:
- green: bfloat16 [4, 8, 3, 2, 384, 384], P('energy', 'slab'), may hold values from -0.3125 to 0.3125
- sigma: bfloat16 [4, 8, 3, 2, 384, 384], P('energy', 'slab'), may hold values from -4 to 4
- phonon: bfloat16 [4, 8, 2, 384, 384], P('energy', 'slab'), may hold values from -4 to 4
- pair_off: int32 [8, 3], replicated, may hold values from -2 to 2, as said below
- pair_count: int32 [8], replicated, may hold values from 1 to 3, as said below
- pair_range: int32 [8, 3], replicated, may hold values from 96 to 384, as said below
Outputs:
- lesser: float32 [4, 8, 2, 384, 384], P('energy', 'slab')
The draws below stay inside these ranges and needn't reach their ends.
Inputs may be any that keep to these rules, and one draw needn't show every extreme that they name: The partner slab k + pair_off[k, q] lies inside the grid. `pair_count`: some slab has 3 live slots. `pair_range`: a multiple of 96; some pair couples all 384 orbitals.
All inputs are finite; a program needn't handle non-finite values.
Results may differ from the reference program's by a relative error of at most 0.0035.
Values may be sent and summed in bfloat16 or wider, within the bound.
A program may use at most 64 MiB of HBM per device.

```python
import jax
import jax.numpy as jnp
from jax import lax

ORB = 384
MAXP = 3
NSLAB = 8
EN = 4


def draw_pair_off(key, part):
    shifts = jax.random.randint(key, (NSLAB, MAXP), -2, 3).astype(jnp.int32)
    slab_ids = jnp.arange(NSLAB, dtype=jnp.int32)[:, None]
    partner = slab_ids + shifts
    outside = (partner < 0) | (partner >= NSLAB)
    return jnp.where(outside, -shifts, shifts).astype(jnp.int32)


def draw_pair_count(key, part):
    counts = jax.random.randint(jax.random.fold_in(key, 11), (NSLAB,), 1, MAXP + 1).astype(jnp.int32)
    fullest = jax.random.randint(jax.random.fold_in(key, 12), (), 0, NSLAB)
    return counts.at[fullest].set(MAXP).astype(jnp.int32)


def draw_pair_range(key, part):
    quarters = jax.random.randint(jax.random.fold_in(key, 21), (NSLAB, MAXP), 1, 5).astype(jnp.int32)
    widest = jax.random.randint(jax.random.fold_in(key, 22), (), 0, NSLAB)
    quarters = quarters.at[widest, 0].set(4)
    return (quarters * (ORB // 4)).astype(jnp.int32)


def block_levels(own_key, dims, split, low, largest):
    loudness = 1.0
    for dim, parts in split:
        heights = jax.random.uniform(jax.random.fold_in(jax.random.fold_in(own_key, 6), dim), (parts,), jnp.float32, low / len(split), largest / len(split))
        loudness = loudness * jnp.repeat(jnp.exp(heights), dims[dim] // parts).reshape((-1,) + (1,) * (len(dims) - 1 - dim))
    return loudness


def bell_draw(own_key, shape, spread, most, pieces=(), kind=jnp.bfloat16):
    entries = jax.random.normal(own_key, shape, jnp.float32) * spread
    if len(pieces) > 0:
        entries = block_levels(own_key, shape, pieces, -0.22, 0.18) * entries
    return jnp.clip(entries, min=-most, max=most).astype(kind)


def setup_inputs(seed: int = 0) -> dict:
    keys = jax.random.split(jax.random.key(seed), 7)
    green = bell_draw(keys[0], (EN, NSLAB, 3, 2, ORB, ORB), ORB ** -0.5, 0.3125, ((0, 4), (1, 8)))
    sigma = bell_draw(keys[1], (EN, NSLAB, MAXP, 2, ORB, ORB), 0.3, 4.0, ((0, 4), (1, 8)))
    phonon = bell_draw(keys[2], (EN, NSLAB, 2, ORB, ORB), 0.3, 4.0, ((0, 4), (1, 8)))
    pair_off = draw_pair_off(jax.random.fold_in(keys[6], 71), 0)
    pair_count = draw_pair_count(jax.random.fold_in(keys[6], 71), 0)
    pair_range = draw_pair_range(jax.random.fold_in(keys[6], 71), 0)
    return {"green": green, "sigma": sigma, "phonon": phonon, "pair_off": pair_off, "pair_count": pair_count, "pair_range": pair_range}


def conj_sum(source, chosen):
    real = jnp.einsum('qmn,qpn->mp', source[:, 0], chosen[:, 0]) + jnp.einsum('qmn,qpn->mp', source[:, 1], chosen[:, 1])
    imag = jnp.einsum('qmn,qpn->mp', source[:, 1], chosen[:, 0]) - jnp.einsum('qmn,qpn->mp', source[:, 0], chosen[:, 1])
    return real, imag


def complex_times(left, real, imag):
    first = jnp.dot(left[0], real, preferred_element_type=jnp.float32) - jnp.dot(left[1], imag, preferred_element_type=jnp.float32)
    second = jnp.dot(left[0], imag, preferred_element_type=jnp.float32) + jnp.dot(left[1], real, preferred_element_type=jnp.float32)
    return jnp.stack([first, second])


def reference(green, sigma, phonon, pair_off, pair_count, pair_range):
    slab_total = green.shape[1]
    width = green.shape[-1]
    slots = pair_off.shape[1]
    positions = jnp.arange(width, dtype=jnp.int32)
    inside = positions[None, None, :] < pair_range[:, :, None]
    square = inside[:, :, :, None] & inside[:, :, None, :]
    masked = jnp.where(square[None, :, :, None], sigma, jnp.zeros((), jnp.bfloat16))
    padded = jnp.pad(phonon.astype(jnp.float32), ((1, 1), (0, 0), (0, 0), (0, 0), (0, 0)))
    phonon_mix = (0.5 * (padded[:-2] + padded[2:])).astype(jnp.bfloat16)
    sources = jnp.concatenate([masked, phonon_mix[:, :, None]], axis=2)
    slot_ids = jnp.arange(slots, dtype=jnp.int32)

    def one_row(flat):
        energy = flat // slab_total
        slab = flat % slab_total
        green_row = green[energy, slab]
        running = jnp.zeros((2, width, width), jnp.float32)
        for delta in (-1, 0, 1):
            other = (slab + delta).astype(jnp.int32)
            clipped = jnp.clip(other, 0, slab_total - 1).astype(jnp.int32)
            valid = (other >= 0) & (other < slab_total)
            source = sources[energy, clipped].astype(jnp.float32)
            offsets = pair_off[clipped]
            count = pair_count[clipped]
            place = (clipped + offsets - slab + 1).astype(jnp.int32)
            usable = (place >= 0) & (place <= 2) & (slot_ids < count)
            pick = jnp.concatenate([jnp.clip(place, 0, 2).astype(jnp.int32), jnp.array([delta + 1], jnp.int32)])
            keep = jnp.concatenate([usable, jnp.array([True])]).astype(jnp.float32)
            chosen = green_row[pick].astype(jnp.float32) * keep[:, None, None, None]
            real, imag = conj_sum(source, chosen)
            term = complex_times(green_row[delta + 1], real.astype(jnp.bfloat16), imag.astype(jnp.bfloat16))
            running = running + jnp.where(valid, term, jnp.zeros_like(term))
        return running

    flat_ids = jnp.arange(green.shape[0] * slab_total, dtype=jnp.int32)
    result = lax.map(one_row, flat_ids)
    return result.reshape(green.shape[0], slab_total, 2, width, width)
```

```python
import functools

import jax
import jax.numpy as jnp
from jax import lax
from jax.experimental import pallas as pl
from jax.experimental.pallas import tpu as pltpu
from jax.sharding import PartitionSpec as P

PIECES = 4


def kernel(
    slabs,
    energies,
    off_ref,
    count_ref,
    range_ref,
    green_hbm,
    sigma_hbm,
    phonon_hbm,
    out_ref,
    green_v,
    own,
    near,
    far,
    sides,
    right,
    left,
    total,
    inner,
    send_near,
    recv_near,
    send_far,
    recv_far,
    send_side,
    recv_side,
    load_sem,
):
    i = lax.axis_index("slab")
    e = lax.axis_index("energy")
    slots = sigma_hbm.shape[0]
    width = green_v.shape[-1]
    half = width // 2
    odd = lax.rem(i, 2)
    step = 1 - 2 * odd
    partner = i + step
    onward = lax.rem(i + 2 * step + slabs, slabs)
    source = lax.rem(i - 2 * step + slabs, slabs)
    up = lax.rem(e + 1, energies)
    down = lax.rem(e - 1 + energies, energies)

    def piece(ref, unit, c):
        return ref.at[unit, c // 2, pl.ds((c % 2) * half, half)]

    def near_copy(src, unit, c):
        return pltpu.make_async_remote_copy(
            src_ref=piece(src, unit, c),
            dst_ref=piece(near, unit, c),
            send_sem=send_near.at[unit, c],
            recv_sem=recv_near.at[unit, c],
            device_id={"slab": partner},
            device_id_type=pl.DeviceIdType.MESH,
        )

    def far_copy(unit, c):
        return pltpu.make_async_remote_copy(
            src_ref=piece(near, unit, c),
            dst_ref=piece(far, unit, c),
            send_sem=send_far.at[unit, c],
            recv_sem=recv_far.at[unit, c],
            device_id={"slab": onward},
            device_id_type=pl.DeviceIdType.MESH,
        )

    def side_copy(place, target):
        return pltpu.make_async_remote_copy(
            src_ref=phonon_hbm,
            dst_ref=sides.at[place],
            send_sem=send_side.at[place],
            recv_sem=recv_side.at[place],
            device_id={"energy": target},
            device_id_type=pl.DeviceIdType.MESH,
        )

    loads = [
        pltpu.make_async_copy(green_hbm, green_v, load_sem.at[0]),
        pltpu.make_async_copy(sigma_hbm, own.at[pl.ds(0, slots)], load_sem.at[1]),
    ]
    for load in loads:
        load.start()

    barrier = pltpu.get_barrier_semaphore()
    for target in (partner, onward, source):
        pl.semaphore_signal(
            barrier, inc=1, device_id={"slab": target}, device_id_type=pl.DeviceIdType.MESH
        )
    for target in (up, down):
        pl.semaphore_signal(
            barrier, inc=1, device_id={"energy": target}, device_id_type=pl.DeviceIdType.MESH
        )
    pl.semaphore_wait(barrier, 5)

    for unit in range(slots):
        for c in range(PIECES):
            near_copy(sigma_hbm, unit, c).start()
    above = side_copy(0, up)
    below = side_copy(1, down)
    above.start()
    below.start()

    loads[0].wait()
    for place in range(3):
        real = green_v[place, 0]
        imag = green_v[place, 1]
        left[place, :, :width] = real
        left[place, :, width:] = imag
        real_t = real.T
        imag_t = imag.T
        right[place, :width, :width] = real_t
        right[place, width:, :width] = imag_t
        right[place, :width, width:] = -imag_t
        right[place, width:, width:] = real_t
    loads[1].wait()

    rows = lax.broadcasted_iota(jnp.int32, (width, width), 0)
    cols = lax.broadcasted_iota(jnp.int32, (width, width), 1)
    furthest = jnp.maximum(rows, cols)
    tile = 2 * width // 3

    def add_unit(where, buffer, delta, unit):
        k = i + delta
        valid = (k >= 0) & (k < slabs)
        k = jnp.clip(k, 0, slabs - 1)
        slot = jnp.minimum(unit, slots - 1)
        mixed = unit == slots
        place = jnp.where(mixed, delta + 1, k + off_ref[slot, k] - i + 1)
        usable = valid & (mixed | ((place >= 0) & (place <= 2) & (slot < count_ref[k])))
        pick = jnp.clip(place, 0, 2)
        reach = jnp.where(mixed, width, range_ref[slot, k])
        reach = jnp.where(usable, reach, 0)
        inside = furthest < reach
        zero = jnp.zeros((), jnp.bfloat16)
        both = jnp.concatenate(
            [jnp.where(inside, buffer[unit, 0], zero), jnp.where(inside, buffer[unit, 1], zero)],
            axis=1,
        )
        for n in range(3):
            span = slice(n * tile, (n + 1) * tile)
            total[where, :, span] += jnp.dot(
                both, right[pick, :, span], preferred_element_type=jnp.float32
            )

    def finish(where, delta, first):
        mine = total[where].astype(jnp.bfloat16)
        inner[:width, :] = mine
        inner[width:, :width] = -mine[:, width:]
        inner[width:, width:] = mine[:, :width]
        place = jnp.clip(delta + 1, 0, 2)
        for part in range(2):
            value = jnp.dot(
                left[place],
                inner[:, part * width : (part + 1) * width],
                preferred_element_type=jnp.float32,
            )
            if first:
                out_ref[part] = value
            else:
                out_ref[part] += value

    def pass_on(unit, c):
        near_copy(own, unit, c).wait_recv()
        far_copy(unit, c).start()

    total[...] = jnp.zeros_like(total)
    for c in range(PIECES // 2):
        pass_on(0, c)

    def one_unit(unit, carry):
        for c in range(PIECES // 2, PIECES):
            pass_on(unit, c)

        @pl.when(unit == 1)
        def _():
            side_copy(0, up).wait_recv()
            side_copy(1, down).wait_recv()
            for part in range(2):
                low = jnp.where(e > 0, sides[0, part].astype(jnp.float32), 0.0)
                high = jnp.where(e < energies - 1, sides[1, part].astype(jnp.float32), 0.0)
                own[slots, part] = (0.5 * (low + high)).astype(jnp.bfloat16)

        add_unit(1, near, step, unit)
        add_unit(0, own, 0, unit)

        @pl.when(unit == 1)
        def _():
            for c in range(PIECES):
                near_copy(own, slots, c).start()

        @pl.when(unit < slots)
        def _():
            for c in range(PIECES // 2):
                pass_on(unit + 1, c)

        @pl.when(unit == slots)
        def _():
            finish(0, 0, True)
            finish(1, step, False)

        for c in range(PIECES):
            far_copy(unit, c).wait_recv()
        add_unit(2, far, -step, unit)
        return carry

    lax.fori_loop(0, slots + 1, one_unit, 0)
    finish(2, -step, False)

    above.wait_send()
    below.wait_send()
    for unit in range(slots + 1):
        for c in range(PIECES):
            near_copy(sigma_hbm if unit < slots else own, unit, c).wait_send()
            far_copy(unit, c).wait_send()


def body(slabs, energies, green, sigma, phonon, pair_off, pair_count, pair_range):
    width = green.shape[-1]
    slots = sigma.shape[2]
    hbm = pl.BlockSpec(memory_space=pl.ANY)
    smem = pl.BlockSpec(memory_space=pltpu.SMEM)
    units = slots + 1
    block = (2, width, width)
    result = pl.pallas_call(
        functools.partial(kernel, slabs, energies),
        out_shape=jax.ShapeDtypeStruct(block, jnp.float32),
        in_specs=[smem, smem, smem, hbm, hbm, hbm],
        out_specs=pl.BlockSpec(memory_space=pltpu.VMEM),
        scratch_shapes=[
            pltpu.VMEM((3,) + block, jnp.bfloat16),
            pltpu.VMEM((units,) + block, jnp.bfloat16),
            pltpu.VMEM((units,) + block, jnp.bfloat16),
            pltpu.VMEM((units,) + block, jnp.bfloat16),
            pltpu.VMEM((2,) + block, jnp.bfloat16),
            pltpu.VMEM((3, 2 * width, 2 * width), jnp.bfloat16),
            pltpu.VMEM((3, width, 2 * width), jnp.bfloat16),
            pltpu.VMEM((3, width, 2 * width), jnp.float32),
            pltpu.VMEM((2 * width, 2 * width), jnp.bfloat16),
            pltpu.SemaphoreType.DMA((units, PIECES)),
            pltpu.SemaphoreType.DMA((units, PIECES)),
            pltpu.SemaphoreType.DMA((units, PIECES)),
            pltpu.SemaphoreType.DMA((units, PIECES)),
            pltpu.SemaphoreType.DMA((2,)),
            pltpu.SemaphoreType.DMA((2,)),
            pltpu.SemaphoreType.DMA((2,)),
        ],
        compiler_params=pltpu.CompilerParams(collective_id=0, has_side_effects=True),
    )(pair_off.T, pair_count, pair_range.T, green[0, 0], sigma[0, 0], phonon[0, 0])
    return result[None, None]


def solution(mesh):
    in_specs = (
        P("energy", "slab", None, None, None, None),
        P("energy", "slab", None, None, None, None),
        P("energy", "slab", None, None, None),
        P(),
        P(),
        P(),
    )
    out_specs = P("energy", "slab", None, None, None)
    run = functools.partial(body, mesh.shape["slab"], mesh.shape["energy"])
    return jax.shard_map(run, mesh=mesh, in_specs=in_specs, out_specs=out_specs, check_vma=False)
```

```python
import functools

import jax
import jax.numpy as jnp
from jax import lax
from jax.experimental import pallas as pl
from jax.experimental.pallas import tpu as pltpu
from jax.sharding import PartitionSpec as P

STRIPS = 4
OFFSETS = (-2, -1, 1, 2)
MESH = pl.DeviceIdType.MESH


def strip_counts(off_ref, count_ref, range_ref, k, strip):
    slots = off_ref.shape[0]
    counts = []
    for offset in OFFSETS:
        most = jnp.int32(0)
        for q in range(slots):
            used = (off_ref[q, k] == offset) & (q < count_ref[k])
            most = jnp.maximum(most, jnp.where(used, (range_ref[q, k] + strip - 1) // strip, 0))
        counts.append(most)
    return counts


def choose(slabs, strip, sizes, off_ref, count_ref, range_ref, out_ref):
    def one(k, most):
        return jnp.maximum(most, sum(strip_counts(off_ref, count_ref, range_ref, k, strip)))

    most = lax.fori_loop(0, slabs, one, jnp.int32(0))
    out_ref[0] = sum(jnp.where(most > size, 1, 0) for size in sizes[:-1])


def kernel(
    slabs,
    energies,
    packed,
    off_ref,
    count_ref,
    range_ref,
    green_hbm,
    sigma_hbm,
    phonon_hbm,
    out_ref,
    green_v,
    sigma_v,
    own,
    near,
    far,
    own_mid,
    near_mid,
    far_mid,
    sides,
    right,
    left,
    whole,
    total,
    inner,
    send_near,
    recv_near,
    send_far,
    recv_far,
    send_side,
    recv_side,
    load_sem,
):
    i = lax.axis_index("slab")
    e = lax.axis_index("energy")
    slots = sigma_hbm.shape[0]
    width = green_v.shape[-1]
    strip = width // STRIPS
    step = 1 - 2 * lax.rem(i, 2)
    partner = i + step
    goes = (i + 2 * step >= 0) & (i + 2 * step < slabs)
    comes = (i - 2 * step >= 0) & (i - 2 * step < slabs)
    onward = lax.rem(i + 2 * step + slabs, slabs)
    source = lax.rem(i - 2 * step + slabs, slabs)
    up = lax.rem(e + 1, energies)
    down = lax.rem(e - 1 + energies, energies)

    def at(main, middle, j):
        return main.at[j] if j < packed else middle.at[j - packed]

    def near_copy(j):
        return pltpu.make_async_remote_copy(
            src_ref=at(own, own_mid, j),
            dst_ref=at(near, near_mid, j),
            send_sem=send_near.at[j],
            recv_sem=recv_near.at[j],
            device_id={"slab": partner},
            device_id_type=MESH,
        )

    def far_copy(j):
        return pltpu.make_async_remote_copy(
            src_ref=at(near, near_mid, j),
            dst_ref=at(far, far_mid, j),
            send_sem=send_far.at[j],
            recv_sem=recv_far.at[j],
            device_id={"slab": onward},
            device_id_type=MESH,
        )

    def side_copy(place, target):
        return pltpu.make_async_remote_copy(
            src_ref=phonon_hbm,
            dst_ref=sides.at[place],
            send_sem=send_side.at[place],
            recv_sem=recv_side.at[place],
            device_id={"energy": target},
            device_id_type=MESH,
        )

    loads = [
        pltpu.make_async_copy(sigma_hbm, sigma_v, load_sem.at[0]),
        pltpu.make_async_copy(green_hbm, green_v, load_sem.at[1]),
    ]
    for load in loads:
        load.start()

    barrier = pltpu.get_barrier_semaphore()
    for target in (partner, onward, source):
        pl.semaphore_signal(barrier, inc=1, device_id={"slab": target}, device_id_type=MESH)
    for target in (up, down):
        pl.semaphore_signal(barrier, inc=1, device_id={"energy": target}, device_id_type=MESH)

    rows = lax.broadcasted_iota(jnp.int32, (strip, width), 0)
    cols = lax.broadcasted_iota(jnp.int32, (strip, width), 1)

    def table(k):
        counts = strip_counts(off_ref, count_ref, range_ref, k, strip)
        bases = [jnp.int32(0)]
        for count in counts[:-1]:
            bases.append(bases[-1] + count)
        return counts, bases

    own_counts, own_bases = table(i)

    def merged(offset, at_row, part, value):
        furthest = jnp.maximum(rows + at_row * strip, cols)
        for q in range(slots):
            used = (off_ref[q, i] == offset) & (q < count_ref[i])
            reach = jnp.where(used, range_ref[q, i], 0)
            value += jnp.where(furthest < reach, sigma_v[q, part, at_row].astype(jnp.float32), 0.0)
        return value.astype(jnp.bfloat16)

    def pack(j):
        offset = jnp.int32(9)
        at_row = jnp.int32(0)
        for o, count, base in zip(OFFSETS, own_counts, own_bases):
            here = (j >= base) & (j < base + count)
            offset = jnp.where(here, o, offset)
            at_row = jnp.where(here, j - base, at_row)
        at_row = jnp.clip(at_row, 0, STRIPS - 1)
        for part in range(2):
            own[j, part] = merged(offset, at_row, part, jnp.zeros((strip, width), jnp.float32))

    loads[0].wait()
    for j in range(2):
        pack(j)
    pl.semaphore_wait(barrier, 5)

    @pl.when(e < energies - 1)
    def _():
        side_copy(0, up).start()

    @pl.when(e > 0)
    def _():
        side_copy(1, down).start()

    for j in range(2, packed):
        pack(j)
        near_copy(j - 2).start()

    loads[1].wait()
    for place in range(3):
        real = green_v[place, 0]
        imag = green_v[place, 1]
        left[place, :, :width] = real
        left[place, :, width:] = imag
        real_t = real.T
        imag_t = imag.T
        right[place, :width, :width] = real_t
        right[place, width:, :width] = imag_t
        right[place, :width, width:] = -imag_t
        right[place, width:, width:] = real_t
        if place == 0:
            near_copy(packed - 2).start()
            near_copy(packed - 1).start()

    tile = 2 * width // 3

    def multiply(where, place):
        for n in range(3):
            span = slice(n * tile, (n + 1) * tile)
            total[where, :, span] += jnp.dot(
                whole[...], right[place, :, span], preferred_element_type=jnp.float32
            )

    def add_packed(where, buffer, delta):
        k = jnp.clip(i + delta, 0, slabs - 1)
        counts, bases = table(k)
        for m in range(2):
            if where == 0:
                place = jnp.int32(2 * m)
            else:
                place = m + jnp.where(delta < 0, 1, 0)
            offset = place - 1 - delta
            count = jnp.int32(0)
            base = jnp.int32(0)
            for o, some, start in zip(OFFSETS, counts, bases):
                count = jnp.where(offset == o, some, count)
                base = jnp.where(offset == o, start, base)
            for s in range(STRIPS):
                inside = jnp.where(s < count, width, 0)
                j = jnp.clip(base + s, 0, packed - 1)
                for part in range(2):
                    whole[s * strip : (s + 1) * strip, part * width : (part + 1) * width] = (
                        jnp.where(cols < inside, buffer[j, part], jnp.zeros((), jnp.bfloat16))
                    )
            multiply(where, place)

    def add_middle(where, buffer, delta):
        for s in range(STRIPS):
            for part in range(2):
                whole[s * strip : (s + 1) * strip, part * width : (part + 1) * width] = buffer[
                    s, part
                ]
        multiply(where, delta + 1)

    def finish(where, delta, first):
        mine = total[where].astype(jnp.bfloat16)
        inner[:width, :] = mine
        inner[width:, :width] = -mine[:, width:]
        inner[width:, width:] = mine[:, :width]
        for part in range(2):
            value = jnp.dot(
                left[delta + 1],
                inner[:, part * width : (part + 1) * width],
                preferred_element_type=jnp.float32,
            )
            if first:
                out_ref[part] = value
            else:
                out_ref[part] += value

    def pass_on(j):
        near_copy(j).wait_recv()

        @pl.when(goes)
        def _():
            far_copy(j).start()

    def mix():
        @pl.when(e > 0)
        def _():
            side_copy(0, up).wait_recv()

        @pl.when(e == 0)
        def _():
            sides[0] = jnp.zeros(sides.shape[1:], sides.dtype)

        @pl.when(e < energies - 1)
        def _():
            side_copy(1, down).wait_recv()

        @pl.when(e == energies - 1)
        def _():
            sides[1] = jnp.zeros(sides.shape[1:], sides.dtype)

        for s in range(STRIPS):
            for part in range(2):
                mixed = 0.5 * (
                    sides[0, part, s].astype(jnp.float32) + sides[1, part, s].astype(jnp.float32)
                )
                mixed = mixed.astype(jnp.bfloat16).astype(jnp.float32)
                own_mid[s, part] = merged(0, s, part, mixed)

    total[...] = jnp.zeros_like(total)
    for j in range(packed):
        pass_on(j)
        if j == 0:
            add_packed(0, own, 0)
        if j == 2:
            mix()
        if j == 3:
            add_middle(0, own_mid, 0)
            for s in range(STRIPS):
                near_copy(packed + s).start()
        if j == 4:
            finish(0, 0, True)

    pass_on(packed)
    add_packed(1, near, step)
    for s in range(1, STRIPS - 1):
        pass_on(packed + s)

    @pl.when(comes)
    def _():
        for j in range(packed):
            far_copy(j).wait_recv()
        add_packed(2, far, -step)

    pass_on(packed + STRIPS - 1)
    add_middle(1, near_mid, step)
    finish(1, step, False)

    @pl.when(comes)
    def _():
        for s in range(STRIPS):
            far_copy(packed + s).wait_recv()
        add_middle(2, far_mid, -step)
        finish(2, -step, False)

    @pl.when(e < energies - 1)
    def _():
        side_copy(0, up).wait_send()

    @pl.when(e > 0)
    def _():
        side_copy(1, down).wait_send()

    for j in range(packed + STRIPS):
        near_copy(j).wait_send()

    @pl.when(goes)
    def _():
        for j in range(packed + STRIPS):
            far_copy(j).wait_send()


def body(slabs, energies, green, sigma, phonon, pair_off, pair_count, pair_range):
    width = green.shape[-1]
    slots = sigma.shape[2]
    strip = width // STRIPS
    hbm = pl.BlockSpec(memory_space=pl.ANY)
    smem = pl.BlockSpec(memory_space=pltpu.SMEM)
    most = STRIPS * min(slots, len(OFFSETS))
    sizes = (most // 2, 2 * most // 3, most)
    block = (2, width, width)
    cut = (2, strip, width)
    tables = (pair_off.T, pair_count, pair_range.T)

    def run(size):
        packed = sizes[size]
        moves = packed + STRIPS
        return pl.pallas_call(
            functools.partial(kernel, slabs, energies, packed),
            out_shape=jax.ShapeDtypeStruct(block, jnp.float32),
            in_specs=[smem, smem, smem, hbm, hbm, hbm],
            out_specs=pl.BlockSpec(memory_space=pltpu.VMEM),
            scratch_shapes=[
                pltpu.VMEM((3,) + block, jnp.bfloat16),
                pltpu.VMEM((slots, 2, STRIPS, strip, width), jnp.bfloat16),
                pltpu.VMEM((packed,) + cut, jnp.bfloat16),
                pltpu.VMEM((packed,) + cut, jnp.bfloat16),
                pltpu.VMEM((packed,) + cut, jnp.bfloat16),
                pltpu.VMEM((STRIPS,) + cut, jnp.bfloat16),
                pltpu.VMEM((STRIPS,) + cut, jnp.bfloat16),
                pltpu.VMEM((STRIPS,) + cut, jnp.bfloat16),
                pltpu.VMEM((2, 2, STRIPS, strip, width), jnp.bfloat16),
                pltpu.VMEM((3, 2 * width, 2 * width), jnp.bfloat16),
                pltpu.VMEM((3, width, 2 * width), jnp.bfloat16),
                pltpu.VMEM((width, 2 * width), jnp.bfloat16),
                pltpu.VMEM((3, width, 2 * width), jnp.float32),
                pltpu.VMEM((2 * width, 2 * width), jnp.bfloat16),
                pltpu.SemaphoreType.DMA((moves,)),
                pltpu.SemaphoreType.DMA((moves,)),
                pltpu.SemaphoreType.DMA((moves,)),
                pltpu.SemaphoreType.DMA((moves,)),
                pltpu.SemaphoreType.DMA((2,)),
                pltpu.SemaphoreType.DMA((2,)),
                pltpu.SemaphoreType.DMA((2,)),
            ],
            compiler_params=pltpu.CompilerParams(collective_id=size, has_side_effects=True),
        )

    which = pl.pallas_call(
        functools.partial(choose, slabs, strip, sizes),
        out_shape=jax.ShapeDtypeStruct((1,), jnp.int32),
        in_specs=[smem, smem, smem],
        out_specs=smem,
    )(*tables)
    result = lax.switch(
        which[0],
        [run(size) for size in range(len(sizes))],
        *tables,
        green[0, 0],
        sigma[0, 0].reshape(slots, 2, STRIPS, strip, width),
        phonon[0, 0].reshape(2, STRIPS, strip, width),
    )
    return result[None, None]


def solution(mesh):
    in_specs = (
        P("energy", "slab", None, None, None, None),
        P("energy", "slab", None, None, None, None),
        P("energy", "slab", None, None, None),
        P(),
        P(),
        P(),
    )
    out_specs = P("energy", "slab", None, None, None)
    run = functools.partial(body, mesh.shape["slab"], mesh.shape["energy"])
    return jax.shard_map(run, mesh=mesh, in_specs=in_specs, out_specs=out_specs, check_vma=False)
```

```python
import functools

import jax
import jax.numpy as jnp
from jax import lax
from jax.experimental import pallas as pl
from jax.experimental.pallas import tpu as pltpu
from jax.sharding import PartitionSpec as P

STRIPS = 4
OFFSETS = (-2, -1, 1, 2)
LAST = 2
MESH = pl.DeviceIdType.MESH


def strip_counts(off_ref, count_ref, range_ref, k, strip):
    slots = off_ref.shape[0]
    counts = []
    side = 1 - 2 * lax.rem(k, 2)
    for order in OFFSETS:
        offset = order * side
        most = jnp.int32(0)
        for q in range(slots):
            used = (off_ref[q, k] == offset) & (q < count_ref[k])
            most = jnp.maximum(most, jnp.where(used, (range_ref[q, k] + strip - 1) // strip, 0))
        counts.append(most)
    return counts


def choose(slabs, strip, sizes, off_ref, count_ref, range_ref, out_ref):
    def one(k, most):
        counts = strip_counts(off_ref, count_ref, range_ref, k, strip)
        return jnp.maximum(most, jnp.maximum(sum(counts), counts[0] + counts[1] + LAST))

    most = lax.fori_loop(0, slabs, one, jnp.int32(0))
    out_ref[0] = sum(jnp.where(most > size, 1, 0) for size in sizes[:-1])


def kernel(
    slabs,
    energies,
    packed,
    off_ref,
    count_ref,
    range_ref,
    green_hbm,
    sigma_hbm,
    phonon_hbm,
    out_ref,
    green_v,
    sigma_v,
    own,
    near,
    far,
    own_mid,
    near_mid,
    far_mid,
    sides,
    right,
    left,
    whole,
    total,
    inner,
    send_near,
    recv_near,
    send_far,
    recv_far,
    send_side,
    recv_side,
    load_sem,
):
    i = lax.axis_index("slab")
    e = lax.axis_index("energy")
    slots = sigma_hbm.shape[0]
    width = green_v.shape[-1]
    strip = width // STRIPS
    step = 1 - 2 * lax.rem(i, 2)
    partner = i + step
    goes = (i + 2 * step >= 0) & (i + 2 * step < slabs)
    comes = (i - 2 * step >= 0) & (i - 2 * step < slabs)
    onward = lax.rem(i + 2 * step + slabs, slabs)
    source = lax.rem(i - 2 * step + slabs, slabs)
    up = lax.rem(e + 1, energies)
    down = lax.rem(e - 1 + energies, energies)

    def at(main, middle, j):
        return main.at[j] if j < packed else middle.at[j - packed]

    def near_copy(j):
        return pltpu.make_async_remote_copy(
            src_ref=at(own, own_mid, j),
            dst_ref=at(near, near_mid, j),
            send_sem=send_near.at[j],
            recv_sem=recv_near.at[j],
            device_id={"slab": partner},
            device_id_type=MESH,
        )

    def own_copy(j):
        return pltpu.make_async_remote_copy(
            src_ref=own.at[j],
            dst_ref=near.at[j],
            send_sem=send_near.at[j],
            recv_sem=recv_near.at[j],
            device_id={"slab": partner},
            device_id_type=MESH,
        )

    def far_copy(j):
        return pltpu.make_async_remote_copy(
            src_ref=at(near, near_mid, j),
            dst_ref=at(far, far_mid, j),
            send_sem=send_far.at[j],
            recv_sem=recv_far.at[j],
            device_id={"slab": onward},
            device_id_type=MESH,
        )

    def side_copy(place, target):
        return pltpu.make_async_remote_copy(
            src_ref=phonon_hbm,
            dst_ref=sides.at[place],
            send_sem=send_side.at[place],
            recv_sem=recv_side.at[place],
            device_id={"energy": target},
            device_id_type=MESH,
        )

    loads = [
        pltpu.make_async_copy(sigma_hbm, sigma_v, load_sem.at[0]),
        pltpu.make_async_copy(green_hbm, green_v, load_sem.at[1]),
    ]
    for load in loads:
        load.start()

    barrier = pltpu.get_barrier_semaphore()
    for target in (partner, onward, source):
        pl.semaphore_signal(barrier, inc=1, device_id={"slab": target}, device_id_type=MESH)
    for target in (up, down):
        pl.semaphore_signal(barrier, inc=1, device_id={"energy": target}, device_id_type=MESH)

    rows = lax.broadcasted_iota(jnp.int32, (strip, width), 0)
    cols = lax.broadcasted_iota(jnp.int32, (strip, width), 1)

    def table(k):
        counts = strip_counts(off_ref, count_ref, range_ref, k, strip)
        bases = [jnp.int32(0)]
        for count in counts[:-1]:
            bases.append(bases[-1] + count)
        return counts, bases

    own_counts, own_bases = table(i)

    def merged(offset, at_row, part, value):
        furthest = jnp.maximum(rows + at_row * strip, cols)
        for q in range(slots):
            used = (off_ref[q, i] == offset) & (q < count_ref[i])
            reach = jnp.where(used, range_ref[q, i], 0)
            value += jnp.where(furthest < reach, sigma_v[q, part, at_row].astype(jnp.float32), 0.0)
        return value.astype(jnp.bfloat16)

    def pack(j):
        offset = jnp.int32(9)
        at_row = jnp.int32(0)
        for o, count, base in zip(OFFSETS, own_counts, own_bases):
            here = (j >= base) & (j < base + count)
            offset = jnp.where(here, o * step, offset)
            at_row = jnp.where(here, j - base, at_row)
        at_row = jnp.clip(at_row, 0, STRIPS - 1)
        for part in range(2):
            own[j, part] = merged(offset, at_row, part, jnp.zeros((strip, width), jnp.float32))

    loads[0].wait()

    def pack_first(j, carry):
        pack(j)
        return carry

    lax.fori_loop(0, 2, pack_first, 0)
    pl.semaphore_wait(barrier, 5)

    @pl.when(e < energies - 1)
    def _():
        side_copy(0, up).start()

    @pl.when(e > 0)
    def _():
        side_copy(1, down).start()

    def pack_next(j, carry):
        pack(j)

        @pl.when(j - 2 < packed - LAST)
        def _():
            own_copy(j - 2).start()

        return carry

    lax.fori_loop(2, packed, pack_next, 0)

    loads[1].wait()

    def arrange(place, carry):
        real = green_v[place, 0]
        imag = green_v[place, 1]
        left[place, :, :width] = real
        left[place, :, width:] = imag
        real_t = real.T
        imag_t = imag.T
        right[place, :width, :width] = real_t
        right[place, width:, :width] = imag_t
        right[place, :width, width:] = -imag_t
        right[place, width:, width:] = real_t
        return carry

    lax.fori_loop(0, 3, arrange, 0)

    tile = 2 * width // 3

    def multiply(where, place):
        for n in range(3):
            span = slice(n * tile, (n + 1) * tile)
            total[where, :, span] += jnp.dot(
                whole[...], right[place, :, span], preferred_element_type=jnp.float32
            )

    def add_packed(where, buffer, delta):
        k = jnp.clip(i + delta, 0, slabs - 1)
        counts, bases = table(k)
        side = 1 - 2 * lax.rem(k, 2)
        held = buffer.shape[0]

        def one(m, carry):
            if where == 0:
                place = 2 * m
            else:
                place = m + jnp.where(delta < 0, 1, 0)
            offset = place - 1 - delta
            count = jnp.int32(0)
            base = jnp.int32(0)
            for o, some, start in zip(OFFSETS, counts, bases):
                count = jnp.where(offset == o * side, some, count)
                base = jnp.where(offset == o * side, start, base)
            for s in range(STRIPS):
                inside = jnp.where(s < count, width, 0)
                j = jnp.clip(base + s, 0, held - 1)
                for part in range(2):
                    whole[s * strip : (s + 1) * strip, part * width : (part + 1) * width] = (
                        jnp.where(cols < inside, buffer[j, part], jnp.zeros((), jnp.bfloat16))
                    )
            multiply(where, place)
            return carry

        lax.fori_loop(0, 2, one, 0)

    def add_middle(where, buffer, delta):
        for s in range(STRIPS):
            for part in range(2):
                whole[s * strip : (s + 1) * strip, part * width : (part + 1) * width] = buffer[
                    s, part
                ]
        multiply(where, delta + 1)

    def finish(where, delta, first):
        mine = total[where].astype(jnp.bfloat16)
        inner[:width, :] = mine
        inner[width:, :width] = -mine[:, width:]
        inner[width:, width:] = mine[:, :width]
        for part in range(2):
            value = jnp.dot(
                left[delta + 1],
                inner[:, part * width : (part + 1) * width],
                preferred_element_type=jnp.float32,
            )
            if first:
                out_ref[part] = value
            else:
                out_ref[part] += value

    def pass_on(j):
        near_copy(j).wait_recv()

        @pl.when(goes)
        def _():
            far_copy(j).start()

    def mix():
        @pl.when(e > 0)
        def _():
            side_copy(0, up).wait_recv()

        @pl.when(e == 0)
        def _():
            sides[0] = jnp.zeros(sides.shape[1:], sides.dtype)

        @pl.when(e < energies - 1)
        def _():
            side_copy(1, down).wait_recv()

        @pl.when(e == energies - 1)
        def _():
            sides[1] = jnp.zeros(sides.shape[1:], sides.dtype)

        for s in range(STRIPS):
            for part in range(2):
                mixed = 0.5 * (
                    sides[0, part, s].astype(jnp.float32) + sides[1, part, s].astype(jnp.float32)
                )
                mixed = mixed.astype(jnp.bfloat16).astype(jnp.float32)
                own_mid[s, part] = merged(0, s, part, mixed)

    total[...] = jnp.zeros_like(total)
    early = packed - LAST
    for j in range(early):
        pass_on(j)
        if j == 0:
            add_packed(0, own, 0)
        if j == 1:
            mix()
            add_middle(0, own_mid, 0)
            for s in range(STRIPS):
                near_copy(packed + s).start()
            for k in range(early, packed):
                near_copy(k).start()
        if j == 2:
            finish(0, 0, True)

    for s in range(STRIPS - 1):
        pass_on(packed + s)

    @pl.when(comes)
    def _():
        for j in range(early):
            far_copy(j).wait_recv()
        add_packed(2, far, -step)

    pass_on(packed + STRIPS - 1)
    add_middle(1, near_mid, step)

    @pl.when(comes)
    def _():
        for s in range(STRIPS):
            far_copy(packed + s).wait_recv()
        add_middle(2, far_mid, -step)
        finish(2, -step, False)

    for j in range(early, packed):
        near_copy(j).wait_recv()
    add_packed(1, near, step)
    finish(1, step, False)

    @pl.when(e < energies - 1)
    def _():
        side_copy(0, up).wait_send()

    @pl.when(e > 0)
    def _():
        side_copy(1, down).wait_send()

    for j in range(packed + STRIPS):
        near_copy(j).wait_send()

    @pl.when(goes)
    def _():
        for j in list(range(early)) + list(range(packed, packed + STRIPS)):
            far_copy(j).wait_send()


def body(slabs, energies, green, sigma, phonon, pair_off, pair_count, pair_range):
    width = green.shape[-1]
    slots = sigma.shape[2]
    strip = width // STRIPS
    hbm = pl.BlockSpec(memory_space=pl.ANY)
    smem = pl.BlockSpec(memory_space=pltpu.SMEM)
    most = STRIPS * min(slots, len(OFFSETS))
    sizes = tuple(range(most // 2, 3 * most // 4)) + (5 * most // 6, most)
    block = (2, width, width)
    cut = (2, strip, width)
    tables = (pair_off.T, pair_count, pair_range.T)

    def run(size):
        packed = sizes[size]
        moves = packed + STRIPS
        return pl.pallas_call(
            functools.partial(kernel, slabs, energies, packed),
            out_shape=jax.ShapeDtypeStruct(block, jnp.float32),
            in_specs=[smem, smem, smem, hbm, hbm, hbm],
            out_specs=pl.BlockSpec(memory_space=pltpu.VMEM),
            scratch_shapes=[
                pltpu.VMEM((3,) + block, jnp.bfloat16),
                pltpu.VMEM((slots, 2, STRIPS, strip, width), jnp.bfloat16),
                pltpu.VMEM((packed,) + cut, jnp.bfloat16),
                pltpu.VMEM((packed,) + cut, jnp.bfloat16),
                pltpu.VMEM((packed - LAST,) + cut, jnp.bfloat16),
                pltpu.VMEM((STRIPS,) + cut, jnp.bfloat16),
                pltpu.VMEM((STRIPS,) + cut, jnp.bfloat16),
                pltpu.VMEM((STRIPS,) + cut, jnp.bfloat16),
                pltpu.VMEM((2, 2, STRIPS, strip, width), jnp.bfloat16),
                pltpu.VMEM((3, 2 * width, 2 * width), jnp.bfloat16),
                pltpu.VMEM((3, width, 2 * width), jnp.bfloat16),
                pltpu.VMEM((width, 2 * width), jnp.bfloat16),
                pltpu.VMEM((3, width, 2 * width), jnp.float32),
                pltpu.VMEM((2 * width, 2 * width), jnp.bfloat16),
                pltpu.SemaphoreType.DMA((moves,)),
                pltpu.SemaphoreType.DMA((moves,)),
                pltpu.SemaphoreType.DMA((moves,)),
                pltpu.SemaphoreType.DMA((moves,)),
                pltpu.SemaphoreType.DMA((2,)),
                pltpu.SemaphoreType.DMA((2,)),
                pltpu.SemaphoreType.DMA((2,)),
            ],
            compiler_params=pltpu.CompilerParams(collective_id=size, has_side_effects=True),
        )

    which = pl.pallas_call(
        functools.partial(choose, slabs, strip, sizes),
        out_shape=jax.ShapeDtypeStruct((1,), jnp.int32),
        in_specs=[smem, smem, smem],
        out_specs=smem,
    )(*tables)
    result = lax.switch(
        which[0],
        [run(size) for size in range(len(sizes))],
        *tables,
        green[0, 0],
        sigma[0, 0].reshape(slots, 2, STRIPS, strip, width),
        phonon[0, 0].reshape(2, STRIPS, strip, width),
    )
    return result[None, None]


def solution(mesh):
    in_specs = (
        P("energy", "slab", None, None, None, None),
        P("energy", "slab", None, None, None, None),
        P("energy", "slab", None, None, None),
        P(),
        P(),
        P(),
    )
    out_specs = P("energy", "slab", None, None, None)
    run = functools.partial(body, mesh.shape["slab"], mesh.shape["energy"])
    return jax.shard_map(run, mesh=mesh, in_specs=in_specs, out_specs=out_specs, check_vma=False)
```
